32 devices in a mesh: group: 2 (over x), lon: 16 (over z, y, core).
Axes of the slice: x: 2, y: 2, z: 4, core: 2. Of those that a mesh axis runs over, the one named last changes fastest.
Arguments:
- initial_state: bfloat16 [512, 8, 64, 128], P('lon', 'group'), parts along dimension 1, may hold values from -10 to 10
- self_weight: bfloat16 [128, 128], replicated, may hold values from -0.5 to 0.5
- neighbour_weight: bfloat16 [6, 128, 128], replicated, may hold values from -0.5 to 0.5
- edge_bias: float32 [6, 128], replicated, may hold values from -4 to 4
- message_weight: bfloat16 [128, 128], replicated, may hold values from -0.5 to 0.5
- state_weight: bfloat16 [128, 128], replicated, may hold values from -0.375 to 0.375
- inbound_weight: bfloat16 [128, 128], replicated, may hold values from -0.375 to 0.375
- node_bias: float32 [128], replicated, may hold values from -2.5 to 2.5
- output_weight: bfloat16 [128, 128], replicated, may hold values from -0.5 to 0.5
- node_gain: float32 [128], replicated, may hold values from 0.5 to 1.5
Outputs:
- final_state: bfloat16 [512, 8, 64, 128], P('lon', 'group'), parts along dimension 1
- profiles: float32 [8, 64, 128], P('group'), parts along dimension 0
The draws below stay inside these ranges and needn't reach their ends.
There are 2 independent parts, one for each index of `group`. The reference program is written for one: setup_inputs(seed, part) draws one part's arguments, and reference() takes and returns one part's arrays. A program takes and returns all parts, laid end to end along the dimension named above; an argument that names none is the same for every part. Nothing has to cross between parts.
All inputs are finite; a program needn't handle non-finite values.
Results may differ from the reference program's by a relative error of at most 0.0095.
Values may be sent and summed in bfloat16 or wider, within the bound.
A program may use at most 128 MiB of HBM per device.

```python
import math
import jax
import jax.numpy as jnp
from jax import lax

C = 128
NLAT = 4
NRAD = 64
STEPS = 4
NLON = 512


def draw_initial_state(key, part):
    first, second = jax.random.split(key, 2)
    shape = (NLON, NLAT, NRAD, C)
    position = jnp.arange(NLON, dtype=jnp.float32) / NLON
    offset = jnp.clip(2.0 * jax.random.normal(second, (1, 1, NRAD, C), jnp.float32), -3.5, 3.5)
    noise = jnp.clip(jax.random.normal(first, shape, jnp.float32), -2.5, 2.5)
    ramp = jnp.exp(math.log(3.0) * position)
    ramp = ramp / jnp.mean(ramp)
    return jnp.clip(noise + offset * ramp.reshape(NLON, 1, 1, 1), -10.0, 10.0).astype(jnp.bfloat16)


def scatter_about(key, extent, scale, bound, kind=jnp.bfloat16):
    return jnp.clip(scale * jax.random.normal(key, extent, jnp.float32), -bound, bound).astype(kind)


def setup_inputs(seed: int = 0, part: int = 0) -> dict:
    splits = jax.random.split(jax.random.key(seed), 11)
    part_keys = jax.random.split(jax.random.fold_in(splits[10], part), 11)
    return {
        "initial_state": draw_initial_state(jax.random.fold_in(jax.random.fold_in(splits[10], part), 71), part),
        "self_weight": scatter_about(splits[1], (C, C), C ** -0.5, 0.5),
        "neighbour_weight": scatter_about(splits[2], (6, C, C), C ** -0.5, 0.5),
        "edge_bias": scatter_about(splits[3], (6, C), 1.0, 4.0, jnp.float32),
        "message_weight": scatter_about(splits[4], (C, C), C ** -0.5, 0.5),
        "state_weight": scatter_about(splits[5], (C, C), (2 * C) ** -0.5, 0.375),
        "inbound_weight": scatter_about(splits[6], (C, C), (2 * C) ** -0.5, 0.375),
        "node_bias": scatter_about(splits[7], (C,), 0.5, 2.5, jnp.float32),
        "output_weight": scatter_about(splits[8], (C, C), C ** -0.5, 0.5),
        "node_gain": jnp.clip(1.0 + 0.1 * jax.random.normal(splits[9], (C,), jnp.float32), 0.5, 1.5),
    }


def latitude_weights(rows):
    centers = -jnp.pi / 2 + (jnp.arange(rows, dtype=jnp.float32) + 0.5) * (jnp.pi / rows)
    return jnp.cos(centers)

def advance(block, profile, weights):
    self_weight, neighbour_weight, edge_bias, message_weight, state_weight, inbound_weight, node_bias, output_weight, node_gain = weights
    inner = block[1:-1]
    rows = block.shape[1]
    levels = block.shape[2]
    latitude = jnp.arange(rows, dtype=jnp.int32).reshape(1, rows, 1, 1)
    radius = jnp.arange(levels, dtype=jnp.int32).reshape(1, 1, levels, 1)
    north_open = (latitude < rows - 1).astype(jnp.float32)
    south_open = (latitude > 0).astype(jnp.float32)
    upper_open = (radius < levels - 1).astype(jnp.float32)
    lower_open = (radius > 0).astype(jnp.float32)
    neighbours = 2.0 + north_open + south_open + upper_open + lower_open
    own_term = jnp.dot(inner, self_weight, preferred_element_type=jnp.float32)

    def projected(source, index):
        return jnp.dot(source, neighbour_weight[index], preferred_element_type=jnp.float32).astype(jnp.bfloat16)
    east = projected(block, 0)[2:]
    west = projected(block, 1)[:-2]
    north = jnp.pad(projected(inner, 2), ((0, 0), (0, 1), (0, 0), (0, 0)))[:, 1:]
    south = jnp.pad(projected(inner, 3), ((0, 0), (1, 0), (0, 0), (0, 0)))[:, :-1]
    upper = jnp.pad(projected(inner, 4), ((0, 0), (0, 0), (0, 1), (0, 0)))[:, :, 1:]
    lower = jnp.pad(projected(inner, 5), ((0, 0), (0, 0), (1, 0), (0, 0)))[:, :, :-1]
    summed = jax.nn.relu(own_term + east + edge_bias[0]) + jax.nn.relu(own_term + west + edge_bias[1])
    summed = summed + north_open * jax.nn.relu(own_term + north + edge_bias[2])
    summed = summed + south_open * jax.nn.relu(own_term + south + edge_bias[3])
    summed = summed + upper_open * jax.nn.relu(own_term + upper + edge_bias[4])
    summed = summed + lower_open * jax.nn.relu(own_term + lower + edge_bias[5])
    mean_hidden = (summed / neighbours).astype(jnp.bfloat16)
    message = jnp.dot(mean_hidden, message_weight, preferred_element_type=jnp.float32).astype(jnp.bfloat16)
    anomaly = (inner.astype(jnp.float32) - profile).astype(jnp.bfloat16)
    hidden = jnp.dot(anomaly, state_weight, preferred_element_type=jnp.float32)
    hidden = hidden + jnp.dot(message, inbound_weight, preferred_element_type=jnp.float32) + node_bias
    hidden = jax.nn.relu(hidden).astype(jnp.bfloat16)
    output = jnp.dot(hidden, output_weight, preferred_element_type=jnp.float32)
    center = lax.optimization_barrier(jnp.mean(output, axis=-1, keepdims=True))
    spread = lax.optimization_barrier(jnp.mean(jnp.square(output - center), axis=-1, keepdims=True))
    update = (output - center) * lax.rsqrt(spread + 1e-05) * node_gain
    return (inner.astype(jnp.float32) + update).astype(jnp.bfloat16)

def reference(initial_state, self_weight, neighbour_weight, edge_bias, message_weight, state_weight, inbound_weight, node_bias, output_weight, node_gain):
    weights = (self_weight, neighbour_weight, edge_bias, message_weight, state_weight, inbound_weight, node_bias, output_weight, node_gain)
    weight_row = latitude_weights(NLAT).reshape(1, NLAT, 1, 1)
    total_weight = NLON * jnp.sum(latitude_weights(NLAT))
    current = initial_state
    collected = []
    for step in range(STEPS):
        profile = lax.optimization_barrier(jnp.sum(current.astype(jnp.float32) * weight_row, axis=(0, 1))) / total_weight
        collected.append(profile)
        block = jnp.concatenate([current[-1:], current, current[:1]], axis=0)
        current = advance(block, profile, weights)
    return (current, jnp.stack(collected))
```

```python
import functools
import math

import jax
import jax.numpy as jnp
from jax import lax
from jax.experimental import pallas as pl
from jax.experimental.pallas import tpu as pltpu
from jax.sharding import PartitionSpec as P

STEPS = 4
SUB = 16
CHUNK = 8
COLS = 4
PER_DOT = 4
PER_DOT_NODE = 4
F32 = jnp.float32
BF16 = jnp.bfloat16


def latitude_weights(rows):
    return [math.cos(-math.pi / 2 + (j + 0.5) * (math.pi / rows)) for j in range(rows)]


def dot(a, b):
    return jnp.dot(a, b, preferred_element_type=F32)


def kernel(
    devices,
    state_in,
    self_weight,
    neighbour_weight,
    edge_bias,
    message_weight,
    state_weight,
    inbound_weight,
    node_bias,
    output_weight,
    node_gain,
    state_out,
    profiles,
    raw,
    wide,
    ext,
    mean,
    halo,
    carry,
    total_bias,
    inverse,
    w_pair,
    w_hidden,
    w_out,
    w_ones,
    table,
    acc,
    part,
    gathered,
    combined,
    in_sem,
    out_sem,
    halo_send,
    halo_recv,
    rs_send,
    rs_recv,
    ag_send,
    ag_recv,
):
    columns, rows, levels, width = raw.shape
    tiles = levels // SUB
    area = rows * levels
    groups = columns // COLS
    chunks = levels // CHUNK
    copies = devices // chunks
    me = lax.axis_index("lon")
    right, left = lax.rem(me + 1, devices), lax.rem(me + devices - 1, devices)
    mine, which = me // copies, lax.rem(me, copies)
    weights = latitude_weights(rows)
    scale = 1.0 / (columns * devices * sum(weights))

    def peer(offset):
        return lax.rem(me + offset, devices)

    barrier = pltpu.get_barrier_semaphore()
    for offset in range(1, devices):
        pl.semaphore_signal(barrier, inc=1, device_id={"lon": peer(offset)})

    def load(group):
        span = pl.ds(group * COLS, COLS)
        return pltpu.make_async_copy(state_in.at[span], raw.at[span], in_sem.at[group])

    def unload(group):
        span = pl.ds(group * COLS, COLS)
        return pltpu.make_async_copy(raw.at[span], state_out.at[span], out_sem.at[group])

    def order(k):
        return lax.rem(k + groups - 1, groups)

    @pl.loop(0, groups)
    def _(k):
        load(order(k)).start()

    self_w = self_weight[...]
    for pair in range(3):
        w_pair[pair, :width, :width] = self_w
        w_pair[pair, width:, width:] = self_w
        w_pair[pair, width:, :width] = neighbour_weight[2 * pair]
        w_pair[pair, :width, width:] = neighbour_weight[2 * pair + 1]
    w_hidden[:width] = state_weight[...]
    w_hidden[width:] = dot(message_weight[...], inbound_weight[...]).astype(BF16)
    out_w = output_weight[...].astype(F32)
    out_w = (out_w - jnp.mean(out_w, axis=1, keepdims=True)).astype(BF16)
    w_out[...] = jnp.zeros_like(w_out)
    w_out[:width, :width] = out_w
    w_out[width:, width:] = out_w
    w_ones[...] = jnp.zeros_like(w_ones)
    w_ones[:width, :width] = jnp.full((width, width), 1.0 / width, BF16)
    w_ones[width:, width:] = jnp.full((width, width), 1.0 / width, BF16)
    sub = lax.broadcasted_iota(jnp.int32, (SUB, width), 0)
    for j in range(rows):
        for k in range(tiles):
            count = jnp.full((SUB, width), 2.0 + (j < rows - 1) + (j > 0), F32)
            bias = jnp.broadcast_to(edge_bias[0:1] + edge_bias[1:2], (SUB, width))
            if j < rows - 1:
                bias = bias + edge_bias[2:3]
            if j > 0:
                bias = bias + edge_bias[3:4]
            up = jnp.ones((SUB, width), F32)
            down = up
            if k == tiles - 1:
                up = (sub < SUB - 1).astype(F32)
            if k == 0:
                down = (sub > 0).astype(F32)
            total_bias[j, k] = bias + up * edge_bias[4:5] + down * edge_bias[5:6]
            inverse[j, k] = 1.0 / (count + up + down)

    def halo_copies(t):
        return (
            pltpu.make_async_remote_copy(
                src_ref=ext.at[columns],
                dst_ref=halo.at[t, 0],
                send_sem=halo_send.at[t, 0],
                recv_sem=halo_recv.at[t, 0],
                device_id={"lon": right},
            ),
            pltpu.make_async_remote_copy(
                src_ref=ext.at[1],
                dst_ref=halo.at[t, 1],
                send_sem=halo_send.at[t, 1],
                recv_sem=halo_recv.at[t, 1],
                device_id={"lon": left},
            ),
        )

    def start_halo(t):
        for copy in halo_copies(t):
            copy.start()

    def scatter(t, target, source):
        return pltpu.make_async_remote_copy(
            src_ref=part.at[t, target // copies],
            dst_ref=gathered.at[t, source],
            send_sem=rs_send.at[t, target],
            recv_sem=rs_recv.at[t, source],
            device_id={"lon": target},
        )

    def start_scatter(t):
        part[t] = acc[...].reshape(chunks, CHUNK, width)

        @pl.loop(1, devices)
        def _(offset):
            scatter(t, peer(offset), me).start()

    def spread(t, target, source):
        return pltpu.make_async_remote_copy(
            src_ref=combined.at[t, source],
            dst_ref=combined.at[t, source],
            send_sem=ag_send.at[t, target],
            recv_sem=ag_recv.at[t, source],
            device_id={"lon": target * copies + which},
        )

    def combine(t):
        gathered[t, me] = part[t, mine]

        @pl.loop(1, devices)
        def _(offset):
            scatter(t, peer(offset), peer(offset)).wait_recv()

        total = gathered[t, 0]
        for source in range(1, devices):
            total = total + gathered[t, source]
        combined[t, mine] = total * scale

        @pl.loop(1, chunks)
        def _(offset):
            spread(t, lax.rem(mine + offset, chunks), mine).start()

    def finish(t):
        @pl.loop(1, chunks)
        def _(offset):
            other = lax.rem(mine + offset, chunks)
            spread(t, other, other).wait_recv()

        profile = combined[t].reshape(levels, width)
        high = profile.astype(BF16)
        low = (profile - high.astype(F32)).astype(BF16)
        shift = dot(high, state_weight[...]) + dot(low, state_weight[...])
        table[...] = node_bias[...] - shift
        tiled = profile.reshape(tiles, SUB, width)
        for k in range(tiles):
            profiles[t, pl.ds(k, SUB, stride=tiles), :] = tiled[k]

        @pl.loop(1, devices)
        def _(offset):
            scatter(t, peer(offset), me).wait_send()

        @pl.loop(1, chunks)
        def _(offset):
            spread(t, lax.rem(mine + offset, chunks), mine).wait_send()

    def accumulate(fresh):
        for j in range(rows):
            line = fresh[0, j]
            for i in range(1, fresh.shape[0]):
                line = line + fresh[i, j]
            line = line * weights[j]
            added = line if j == 0 else added + line
        acc[...] += added

    acc[...] = jnp.zeros_like(acc)

    @pl.loop(0, groups)
    def _(k):
        group = order(k)
        base = group * COLS
        load(group).wait()

        @pl.when(k == 2)
        def _():
            pl.semaphore_wait(barrier, devices - 1)
            start_halo(0)

        block = raw[pl.ds(base, COLS)].astype(F32).reshape(COLS * rows, levels, width)
        wide[...] = block
        accumulate(
            jnp.concatenate(
                [wide[:, pl.ds(k, SUB, stride=tiles), :] for k in range(tiles)], axis=1
            ).reshape(COLS, rows, levels, width)
        )
        for k in range(tiles):
            piece = wide[:, pl.ds(k, SUB, stride=tiles), :].astype(BF16)
            ext[pl.ds(base + 1, COLS), :, k] = piece.reshape(COLS, rows, SUB, width)

    start_scatter(0)

    def lifted(x, index):
        return jnp.maximum(x, -edge_bias[index : index + 1])

    def edges(t):
        for copy in halo_copies(t):
            copy.wait_recv()
        ext[0] = halo[t, 0]
        ext[columns + 1] = halo[t, 1]
        both = jnp.concatenate([ext[0].reshape(area, width), ext[1].reshape(area, width)], axis=1)
        carry[...] = lifted(dot(both, w_pair[0, :, width:]), 1).reshape(rows, levels, width)

        @pl.loop(0, groups)
        def _(group):
            @pl.when(group == groups // 2)
            def _():
                combine(t)

            for piece in range(COLS // PER_DOT):
                edge_piece(group * COLS + piece * PER_DOT)

        for copy in halo_copies(t):
            copy.wait_send()

    def edge_piece(base):
        n = PER_DOT
        here = ext[pl.ds(base + 1, n)]
        flat = here.reshape(n * area, width)
        ahead = ext[pl.ds(base + 2, n)].reshape(n * area, width)
        x = dot(jnp.concatenate([flat, ahead], axis=1), w_pair[0])
        east = lifted(x[:, :width], 0).reshape(n, rows, levels, width)
        west = lifted(x[:, width:], 1).reshape(n, rows, levels, width)
        west = jnp.concatenate([carry[...][None], west], axis=0)
        carry[...] = west[n]
        longitude = east + west[:n]

        lower = here[:, :-1].reshape(n * (area - levels), width)
        upper = here[:, 1:].reshape(n * (area - levels), width)
        x = dot(jnp.concatenate([lower, upper], axis=1), w_pair[1])
        north = lifted(x[:, :width], 2).reshape(n, rows - 1, levels, width)
        south = lifted(x[:, width:], 3).reshape(n, rows - 1, levels, width)

        tile = here.reshape(n * rows, tiles, SUB, width)
        first = tile[:, 0].astype(F32)
        first = pltpu.roll(first, SUB - 1, 1).astype(BF16).reshape(n * rows, 1, SUB, width)
        above = jnp.concatenate([tile[:, 1:], first], axis=1).reshape(n * area, width)
        x = dot(jnp.concatenate([flat, above], axis=1), w_pair[2])
        up = lifted(x[:, :width], 4).reshape(n * rows, tiles, SUB, width)
        down = lifted(x[:, width:], 5).reshape(n * rows, tiles, SUB, width)
        row = lax.broadcasted_iota(jnp.int32, (1, SUB, width), 1)
        last = jnp.where(row < SUB - 1, up[:, tiles - 1], 0.0)
        wrapped = jnp.where(row > 0, pltpu.roll(down[:, tiles - 1], 1, 1), 0.0)
        for k in range(tiles):
            r = (up[:, k] if k < tiles - 1 else last) + (down[:, k - 1] if k > 0 else wrapped)
            r = r.reshape(n, rows, SUB, width)
            span = slice(k * SUB, (k + 1) * SUB)
            for j in range(rows):
                s = longitude[:, j, span] + r[:, j]
                if j < rows - 1:
                    s = s + north[:, j, span]
                if j > 0:
                    s = s + south[:, j - 1, span]
                s = (s + total_bias[j, k]) * inverse[j, k]
                mean[pl.ds(base, n), j, k] = s.astype(BF16)

    def nodes(t, last):
        acc[...] = jnp.zeros_like(acc)

        @pl.loop(0, groups)
        def _(k):
            if not last:

                @pl.when(k == 2)
                def _():
                    start_halo(t + 1)

            group = order(k)
            for piece in range(COLS // PER_DOT_NODE):
                node_piece(group * COLS + piece * PER_DOT_NODE, last)
            if last:
                unload(group).start()

        if not last:
            start_scatter(t + 1)

    def node_piece(base, last):
        n = PER_DOT_NODE
        size = n * area
        here = ext[pl.ds(base + 1, n)].reshape(size, width)
        inbound = mean[pl.ds(base, n)].reshape(size, width)
        hidden = dot(jnp.concatenate([here, inbound], axis=1), w_hidden[...])
        hidden = hidden.reshape(n * rows, levels, width) + table[...]
        hidden = jnp.maximum(hidden, 0.0).astype(BF16).reshape(size, width)
        half = size // 2
        out = dot(jnp.concatenate([hidden[:half], hidden[half:]], axis=1), w_out[...])
        spread_ = dot((out * out).astype(BF16), w_ones[...])
        factor = lax.rsqrt(spread_ + 1e-05)
        gain = node_gain[...]
        gain = jnp.concatenate([gain, gain], axis=1)
        update = out * factor * gain
        update = jnp.concatenate([update[:, :width], update[:, width:]], axis=0)
        fresh = here.astype(F32) + update
        if last:
            tiled = fresh.reshape(n * rows, tiles, SUB, width)
            for k in range(tiles):
                wide[: n * rows, pl.ds(k, SUB, stride=tiles), :] = tiled[:, k]
            whole = wide[: n * rows].astype(BF16)
            raw[pl.ds(base, n)] = whole.reshape(n, rows, levels, width)
        else:
            ext[pl.ds(base + 1, n)] = fresh.astype(BF16).reshape(n, rows, tiles, SUB, width)
            accumulate(fresh.reshape(n, rows, levels, width))

    @pl.loop(0, STEPS - 1)
    def _(t):
        edges(t)
        finish(t)
        nodes(t, False)

    edges(STEPS - 1)
    finish(STEPS - 1)
    nodes(STEPS - 1, True)

    @pl.loop(0, groups)
    def _(group):
        unload(group).wait()


def body(
    initial_state,
    self_weight,
    neighbour_weight,
    edge_bias,
    message_weight,
    state_weight,
    inbound_weight,
    node_bias,
    output_weight,
    node_gain,
):
    columns, rows, levels, width = initial_state.shape
    devices = lax.axis_size("lon")
    tiles = levels // SUB
    groups = columns // COLS
    chunks = levels // CHUNK
    vmem = pl.BlockSpec(memory_space=pltpu.VMEM)
    hbm = pl.BlockSpec(memory_space=pl.ANY)
    dma = pltpu.SemaphoreType.DMA
    return pl.pallas_call(
        functools.partial(kernel, devices),
        out_shape=(
            jax.ShapeDtypeStruct(initial_state.shape, BF16),
            jax.ShapeDtypeStruct((STEPS, levels, width), F32),
        ),
        in_specs=[hbm] + [vmem] * 9,
        out_specs=(hbm, vmem),
        scratch_shapes=[
            pltpu.VMEM((columns, rows, levels, width), BF16),
            pltpu.VMEM((COLS * rows, levels, width), F32),
            pltpu.VMEM((columns + 2, rows, tiles, SUB, width), BF16),
            pltpu.VMEM((columns, rows, tiles, SUB, width), BF16),
            pltpu.VMEM((STEPS, 2, rows, tiles, SUB, width), BF16),
            pltpu.VMEM((rows, levels, width), F32),
            pltpu.VMEM((rows, tiles, SUB, width), F32),
            pltpu.VMEM((rows, tiles, SUB, width), F32),
            pltpu.VMEM((3, 2 * width, 2 * width), BF16),
            pltpu.VMEM((2 * width, width), BF16),
            pltpu.VMEM((2 * width, 2 * width), BF16),
            pltpu.VMEM((2 * width, 2 * width), BF16),
            pltpu.VMEM((levels, width), F32),
            pltpu.VMEM((levels, width), F32),
            pltpu.VMEM((STEPS, chunks, CHUNK, width), F32),
            pltpu.VMEM((STEPS, devices, CHUNK, width), F32),
            pltpu.VMEM((STEPS, chunks, CHUNK, width), F32),
            dma((groups,)),
            dma((groups,)),
            dma((STEPS, 2)),
            dma((STEPS, 2)),
            dma((STEPS, devices)),
            dma((STEPS, devices)),
            dma((STEPS, chunks)),
            dma((STEPS, chunks)),
        ],
        compiler_params=pltpu.CompilerParams(
            collective_id=0, has_side_effects=True, vmem_limit_bytes=60 * 1024 * 1024
        ),
    )(
        initial_state,
        self_weight,
        neighbour_weight,
        edge_bias,
        message_weight,
        state_weight,
        inbound_weight,
        node_bias.reshape(1, width),
        output_weight,
        node_gain.reshape(1, width),
    )


def solution(mesh):
    in_specs = (P("lon", "group", None, None), P(), P(), P(), P(), P(), P(), P(), P(), P())
    out_specs = (P("lon", "group", None, None), P("group", None, None))
    return jax.shard_map(body, mesh=mesh, in_specs=in_specs, out_specs=out_specs, check_vma=False)
```

```python
import functools
import math

import jax
import jax.numpy as jnp
from jax import lax
from jax.experimental import pallas as pl
from jax.experimental.pallas import tpu as pltpu
from jax.sharding import PartitionSpec as P

STEPS = 4
SUB = 16
INNER = 4
COLS = 8
PER_DOT = 4
PER_DOT_NODE = 4
F32 = jnp.float32
BF16 = jnp.bfloat16


def latitude_weights(rows):
    return [math.cos(-math.pi / 2 + (j + 0.5) * (math.pi / rows)) for j in range(rows)]


def dot(a, b):
    return jnp.dot(a, b, preferred_element_type=F32)


def kernel(
    devices,
    state_in,
    self_weight,
    neighbour_weight,
    edge_bias,
    message_weight,
    state_weight,
    inbound_weight,
    node_bias,
    output_weight,
    node_gain,
    state_out,
    profiles,
    raw,
    wide,
    ext,
    mean,
    halo,
    carry,
    total_bias,
    inverse,
    w_pair,
    w_hidden,
    w_out,
    w_ones,
    table,
    acc,
    part,
    gathered,
    outer,
    combined,
    in_sem,
    out_sem,
    halo_send,
    halo_recv,
    rs_send,
    rs_recv,
    ex_send,
    ex_recv,
    ag_send,
    ag_recv,
):
    columns, rows, levels, width = raw.shape
    tiles = levels // SUB
    area = rows * levels
    groups = columns // COLS
    outers = devices // INNER
    me = lax.axis_index("lon")
    right, left = lax.rem(me + 1, devices), lax.rem(me + devices - 1, devices)
    group_id, mine = me // INNER, lax.rem(me, INNER)
    weights = latitude_weights(rows)
    scale = 1.0 / (columns * devices * sum(weights))

    def peer(offset):
        return lax.rem(me + offset, devices)

    barrier = pltpu.get_barrier_semaphore()
    for offset in range(1, devices):
        pl.semaphore_signal(barrier, inc=1, device_id={"lon": peer(offset)})

    def load(group):
        span = pl.ds(group * COLS, COLS)
        return pltpu.make_async_copy(state_in.at[span], raw.at[span], in_sem.at[group])

    def unload(group):
        span = pl.ds(group * COLS, COLS)
        return pltpu.make_async_copy(raw.at[span], state_out.at[span], out_sem.at[group])

    def order(k):
        return lax.rem(k + groups - 1, groups)

    @pl.loop(0, groups)
    def _(k):
        load(order(k)).start()

    self_w = self_weight[...]
    for pair in range(3):
        w_pair[pair, :width, :width] = self_w
        w_pair[pair, width:, width:] = self_w
        w_pair[pair, width:, :width] = neighbour_weight[2 * pair]
        w_pair[pair, :width, width:] = neighbour_weight[2 * pair + 1]
    w_hidden[:width] = state_weight[...]
    w_hidden[width:] = dot(message_weight[...], inbound_weight[...]).astype(BF16)
    out_w = output_weight[...].astype(F32)
    out_w = (out_w - jnp.mean(out_w, axis=1, keepdims=True)).astype(BF16)
    w_out[...] = jnp.zeros_like(w_out)
    w_out[:width, :width] = out_w
    w_out[width:, width:] = out_w
    w_ones[...] = jnp.zeros_like(w_ones)
    w_ones[:width, :width] = jnp.full((width, width), 1.0 / width, BF16)
    w_ones[width:, width:] = jnp.full((width, width), 1.0 / width, BF16)
    sub = lax.broadcasted_iota(jnp.int32, (SUB, width), 0)
    for j in range(rows):
        for k in range(tiles):
            count = jnp.full((SUB, width), 2.0 + (j < rows - 1) + (j > 0), F32)
            bias = jnp.broadcast_to(edge_bias[0:1] + edge_bias[1:2], (SUB, width))
            if j < rows - 1:
                bias = bias + edge_bias[2:3]
            if j > 0:
                bias = bias + edge_bias[3:4]
            up = jnp.ones((SUB, width), F32)
            down = up
            if k == tiles - 1:
                up = (sub < SUB - 1).astype(F32)
            if k == 0:
                down = (sub > 0).astype(F32)
            total_bias[j, k] = bias + up * edge_bias[4:5] + down * edge_bias[5:6]
            inverse[j, k] = 1.0 / (count + up + down)

    def halo_copies(t):
        return (
            pltpu.make_async_remote_copy(
                src_ref=ext.at[columns],
                dst_ref=halo.at[t, 0],
                send_sem=halo_send.at[t, 0],
                recv_sem=halo_recv.at[t, 0],
                device_id={"lon": right},
            ),
            pltpu.make_async_remote_copy(
                src_ref=ext.at[1],
                dst_ref=halo.at[t, 1],
                send_sem=halo_send.at[t, 1],
                recv_sem=halo_recv.at[t, 1],
                device_id={"lon": left},
            ),
        )

    def start_halo(t):
        for copy in halo_copies(t):
            copy.start()

    def push(source, target, send, recv, device):
        return pltpu.make_async_remote_copy(
            src_ref=source, dst_ref=target, send_sem=send, recv_sem=recv, device_id={"lon": device}
        )

    def scatter(t, target, source):
        return push(
            part.at[t, target],
            gathered.at[t, source],
            rs_send.at[t, target],
            rs_recv.at[t, source],
            group_id * INNER + target,
        )

    def across(t, target, source):
        return push(
            outer.at[t, source],
            outer.at[t, source],
            ex_send.at[t, target],
            ex_recv.at[t, source],
            target * INNER + mine,
        )

    def spread(t, target, source):
        return push(
            combined.at[t, source],
            combined.at[t, source],
            ag_send.at[t, target],
            ag_recv.at[t, source],
            group_id * INNER + target,
        )

    def inner_peer(offset):
        return lax.rem(mine + offset, INNER)

    def outer_peer(offset):
        return lax.rem(group_id + offset, outers)

    def start_scatter(t):
        part[t] = acc[...].reshape(INNER, levels // INNER, width)
        for offset in range(1, INNER):
            scatter(t, inner_peer(offset), mine).start()

    def combine(t):
        gathered[t, mine] = part[t, mine]
        for offset in range(1, INNER):
            other = inner_peer(offset)
            scatter(t, other, other).wait_recv()
        total = gathered[t, 0]
        for source in range(1, INNER):
            total = total + gathered[t, source]
        outer[t, group_id] = total
        for offset in range(1, outers):
            across(t, outer_peer(offset), group_id).start()

    def combine_outer(t):
        for offset in range(1, outers):
            other = outer_peer(offset)
            across(t, other, other).wait_recv()
        total = outer[t, 0]
        for source in range(1, outers):
            total = total + outer[t, source]
        combined[t, mine] = total * scale
        for offset in range(1, INNER):
            spread(t, inner_peer(offset), mine).start()

    def finish(t):
        for offset in range(1, INNER):
            other = inner_peer(offset)
            spread(t, other, other).wait_recv()

        profile = combined[t].reshape(levels, width)
        high = profile.astype(BF16)
        low = (profile - high.astype(F32)).astype(BF16)
        shift = dot(high, state_weight[...]) + dot(low, state_weight[...])
        table[...] = node_bias[...] - shift
        tiled = profile.reshape(tiles, SUB, width)
        for k in range(tiles):
            profiles[t, pl.ds(k, SUB, stride=tiles), :] = tiled[k]

        for offset in range(1, INNER):
            scatter(t, inner_peer(offset), mine).wait_send()
            spread(t, inner_peer(offset), mine).wait_send()
        for offset in range(1, outers):
            across(t, outer_peer(offset), group_id).wait_send()

    def accumulate(fresh):
        for j in range(rows):
            line = fresh[0, j]
            for i in range(1, fresh.shape[0]):
                line = line + fresh[i, j]
            line = line * weights[j]
            added = line if j == 0 else added + line
        acc[...] += added

    acc[...] = jnp.zeros_like(acc)
    ext[0] = jnp.zeros_like(ext[0])
    ext[columns + 1] = jnp.zeros_like(ext[0])

    @pl.loop(0, groups)
    def _(k):
        group = order(k)
        base = group * COLS
        load(group).wait()

        @pl.when(k == 2)
        def _():
            pl.semaphore_wait(barrier, devices - 1)
            start_halo(0)

        block = raw[pl.ds(base, COLS)].astype(F32).reshape(COLS * rows, levels, width)
        wide[...] = block
        accumulate(
            jnp.concatenate(
                [wide[:, pl.ds(k, SUB, stride=tiles), :] for k in range(tiles)], axis=1
            ).reshape(COLS, rows, levels, width)
        )
        for k in range(tiles):
            piece = wide[:, pl.ds(k, SUB, stride=tiles), :].astype(BF16)
            ext[pl.ds(base + 1, COLS), :, k] = piece.reshape(COLS, rows, SUB, width)

    start_scatter(0)

    def lifted(x, index):
        return jnp.maximum(x, -edge_bias[index : index + 1])

    def edges(t):
        carry[...] = jnp.zeros_like(carry)

        @pl.loop(0, groups)
        def _(group):
            @pl.when(group == groups // 2)
            def _():
                combine(t)

            for piece in range(COLS // PER_DOT):
                edge_piece(group * COLS + piece * PER_DOT, PER_DOT)

        combine_outer(t)
        for copy in halo_copies(t):
            copy.wait_recv()
        ext[0] = halo[t, 0]
        ext[columns + 1] = halo[t, 1]

        @pl.loop(0, 2)
        def _(side):
            base = side * (columns - 1)
            before = ext[base].reshape(area, width)
            both = jnp.concatenate([before, ext[base + 1].reshape(area, width)], axis=1)
            west = lifted(dot(both, w_pair[0, :, width:]), 1)
            carry[...] = west.reshape(rows, levels, width)
            edge_piece(base, 1)

        for copy in halo_copies(t):
            copy.wait_send()

    def edge_piece(base, n):
        here = ext[pl.ds(base + 1, n)]
        flat = here.reshape(n * area, width)
        ahead = ext[pl.ds(base + 2, n)].reshape(n * area, width)
        x = dot(jnp.concatenate([flat, ahead], axis=1), w_pair[0])
        east = lifted(x[:, :width], 0).reshape(n, rows, levels, width)
        west = lifted(x[:, width:], 1).reshape(n, rows, levels, width)
        west = jnp.concatenate([carry[...][None], west], axis=0)
        carry[...] = west[n]
        longitude = east + west[:n]

        lower = here[:, :-1].reshape(n * (area - levels), width)
        upper = here[:, 1:].reshape(n * (area - levels), width)
        x = dot(jnp.concatenate([lower, upper], axis=1), w_pair[1])
        north = lifted(x[:, :width], 2).reshape(n, rows - 1, levels, width)
        south = lifted(x[:, width:], 3).reshape(n, rows - 1, levels, width)

        tile = here.reshape(n * rows, tiles, SUB, width)
        first = tile[:, 0].astype(F32)
        first = pltpu.roll(first, SUB - 1, 1).astype(BF16).reshape(n * rows, 1, SUB, width)
        above = jnp.concatenate([tile[:, 1:], first], axis=1).reshape(n * area, width)
        x = dot(jnp.concatenate([flat, above], axis=1), w_pair[2])
        up = lifted(x[:, :width], 4).reshape(n * rows, tiles, SUB, width)
        down = lifted(x[:, width:], 5).reshape(n * rows, tiles, SUB, width)
        row = lax.broadcasted_iota(jnp.int32, (1, SUB, width), 1)
        last = jnp.where(row < SUB - 1, up[:, tiles - 1], 0.0)
        wrapped = jnp.where(row > 0, pltpu.roll(down[:, tiles - 1], 1, 1), 0.0)
        for k in range(tiles):
            r = (up[:, k] if k < tiles - 1 else last) + (down[:, k - 1] if k > 0 else wrapped)
            r = r.reshape(n, rows, SUB, width)
            span = slice(k * SUB, (k + 1) * SUB)
            for j in range(rows):
                s = longitude[:, j, span] + r[:, j]
                if j < rows - 1:
                    s = s + north[:, j, span]
                if j > 0:
                    s = s + south[:, j - 1, span]
                s = (s + total_bias[j, k]) * inverse[j, k]
                mean[pl.ds(base, n), j, k] = s.astype(BF16)

    def nodes(t, last):
        acc[...] = jnp.zeros_like(acc)

        @pl.loop(0, groups)
        def _(k):
            if not last:

                @pl.when(k == 2)
                def _():
                    start_halo(t + 1)

            group = order(k)
            for piece in range(COLS // PER_DOT_NODE):
                node_piece(group * COLS + piece * PER_DOT_NODE, last)
            if last:
                unload(group).start()

        if not last:
            start_scatter(t + 1)

    def node_piece(base, last):
        n = PER_DOT_NODE
        size = n * area
        here = ext[pl.ds(base + 1, n)].reshape(size, width)
        inbound = mean[pl.ds(base, n)].reshape(size, width)
        hidden = dot(jnp.concatenate([here, inbound], axis=1), w_hidden[...])
        hidden = hidden.reshape(n * rows, levels, width) + table[...]
        hidden = jnp.maximum(hidden, 0.0).astype(BF16).reshape(size, width)
        half = size // 2
        out = dot(jnp.concatenate([hidden[:half], hidden[half:]], axis=1), w_out[...])
        spread_ = dot((out * out).astype(BF16), w_ones[...])
        factor = lax.rsqrt(spread_ + 1e-05)
        gain = node_gain[...]
        gain = jnp.concatenate([gain, gain], axis=1)
        update = out * factor * gain
        update = jnp.concatenate([update[:, :width], update[:, width:]], axis=0)
        fresh = here.astype(F32) + update
        if last:
            tiled = fresh.reshape(n * rows, tiles, SUB, width)
            for k in range(tiles):
                wide[: n * rows, pl.ds(k, SUB, stride=tiles), :] = tiled[:, k]
            whole = wide[: n * rows].astype(BF16)
            raw[pl.ds(base, n)] = whole.reshape(n, rows, levels, width)
        else:
            ext[pl.ds(base + 1, n)] = fresh.astype(BF16).reshape(n, rows, tiles, SUB, width)
            accumulate(fresh.reshape(n, rows, levels, width))

    @pl.loop(0, STEPS - 1)
    def _(t):
        edges(t)
        finish(t)
        nodes(t, False)

    edges(STEPS - 1)
    finish(STEPS - 1)
    nodes(STEPS - 1, True)

    @pl.loop(0, groups)
    def _(group):
        unload(group).wait()


def body(
    initial_state,
    self_weight,
    neighbour_weight,
    edge_bias,
    message_weight,
    state_weight,
    inbound_weight,
    node_bias,
    output_weight,
    node_gain,
):
    columns, rows, levels, width = initial_state.shape
    devices = lax.axis_size("lon")
    tiles = levels // SUB
    groups = columns // COLS
    outers = devices // INNER
    piece = (levels // INNER, width)
    vmem = pl.BlockSpec(memory_space=pltpu.VMEM)
    hbm = pl.BlockSpec(memory_space=pl.ANY)
    dma = pltpu.SemaphoreType.DMA
    return pl.pallas_call(
        functools.partial(kernel, devices),
        out_shape=(
            jax.ShapeDtypeStruct(initial_state.shape, BF16),
            jax.ShapeDtypeStruct((STEPS, levels, width), F32),
        ),
        in_specs=[hbm] + [vmem] * 9,
        out_specs=(hbm, vmem),
        scratch_shapes=[
            pltpu.VMEM((columns, rows, levels, width), BF16),
            pltpu.VMEM((COLS * rows, levels, width), F32),
            pltpu.VMEM((columns + 2, rows, tiles, SUB, width), BF16),
            pltpu.VMEM((columns, rows, tiles, SUB, width), BF16),
            pltpu.VMEM((STEPS, 2, rows, tiles, SUB, width), BF16),
            pltpu.VMEM((rows, levels, width), F32),
            pltpu.VMEM((rows, tiles, SUB, width), F32),
            pltpu.VMEM((rows, tiles, SUB, width), F32),
            pltpu.VMEM((3, 2 * width, 2 * width), BF16),
            pltpu.VMEM((2 * width, width), BF16),
            pltpu.VMEM((2 * width, 2 * width), BF16),
            pltpu.VMEM((2 * width, 2 * width), BF16),
            pltpu.VMEM((levels, width), F32),
            pltpu.VMEM((levels, width), F32),
            pltpu.VMEM((STEPS, INNER, *piece), F32),
            pltpu.VMEM((STEPS, INNER, *piece), F32),
            pltpu.VMEM((STEPS, outers, *piece), F32),
            pltpu.VMEM((STEPS, INNER, *piece), F32),
            dma((groups,)),
            dma((groups,)),
            dma((STEPS, 2)),
            dma((STEPS, 2)),
            dma((STEPS, INNER)),
            dma((STEPS, INNER)),
            dma((STEPS, outers)),
            dma((STEPS, outers)),
            dma((STEPS, INNER)),
            dma((STEPS, INNER)),
        ],
        compiler_params=pltpu.CompilerParams(
            collective_id=0, has_side_effects=True, vmem_limit_bytes=60 * 1024 * 1024
        ),
    )(
        initial_state,
        self_weight,
        neighbour_weight,
        edge_bias,
        message_weight,
        state_weight,
        inbound_weight,
        node_bias.reshape(1, width),
        output_weight,
        node_gain.reshape(1, width),
    )


def solution(mesh):
    in_specs = (P("lon", "group", None, None), P(), P(), P(), P(), P(), P(), P(), P(), P())
    out_specs = (P("lon", "group", None, None), P("group", None, None))
    return jax.shard_map(body, mesh=mesh, in_specs=in_specs, out_specs=out_specs, check_vma=False)
```
